32 devices in a mesh: tile: 8 (over y, x, core), lev: 4 (over z).
Axes of the slice: x: 2, y: 2, z: 4, core: 2. Of those that a mesh axis runs over, the one named last changes fastest.
Arguments:
- members_pert: bfloat16 [64, 16, 32768], P('lev', None, 'tile'), may hold values from -4 to 4
- coarse_pert: bfloat16 [64, 8, 2048], P('lev', None, 'tile'), may hold values from -6 to 6
- member_ctrl: bfloat16 [64, 16, 2048], P('lev', None, 'tile'), may hold values from -6 to 6
- coarse_ctrl: bfloat16 [64, 8, 2048], P('lev', None, 'tile'), may hold values from -6 to 6
- vert_loc: float32 [64, 64], replicated, may hold values from -1.5 to 1.5, as said below
- stencil: int32 [4, 32768], P(None, 'tile'), may hold values from 0 to 383, as said below
- interp_w: bfloat16 [4, 32768], P(None, 'tile'), may hold values from 0 to 1, as said below
Outputs:
- member_out: float32 [64, 16, 2048], P('lev', None, 'tile')
- coarse_out: float32 [64, 8, 2048], P('lev', None, 'tile')
The draws below stay inside these ranges and needn't reach their ends.
Inputs may be any that keep to these rules, and one draw needn't show every extreme that they name: vert_loc[i, j] is zero where |i - j| > 4, and nonzero where |i - j| = 4. stencil indexes a window of 384 coarse cells of the fine cell's tile index: the last 64 coarse cells of the tile index before it (the first one's predecessor is the last), its own 256 cells, then the first 64 cells of the tile index after it; the four corners of a fine cell are distinct. `interp_w`: the four weights of a fine cell are nonnegative and sum to one up to rounding.
All inputs are finite; a program needn't handle non-finite values.
Results may differ from the reference program's by a relative error of at most 0.013.
Values may be sent and summed in bfloat16 or wider, within the bound.
A program may use at most 64 MiB of HBM per device.

```python
import jax
import jax.numpy as jnp
from jax import lax

MEMBERS = 16
COARSE_MEMBERS = 8
HB = 4
CW = 64
CR = 4
LEV = 64
NCD = 256
NFD = 4096
NC = 2048
NF = 32768
N_TILE = 8


def draw_vert_loc(key, part):
    first_key, second_key = jax.random.split(key)
    rows = jnp.arange(LEV, dtype=jnp.int32)[:, None]
    columns = jnp.arange(LEV, dtype=jnp.int32)[None, :]
    distance = jnp.abs(rows - columns)
    offdiag = jnp.clip(0.35 * jax.random.normal(first_key, (LEV, LEV), jnp.float32), -1.5, 1.5)
    offdiag = jnp.where(jnp.abs(offdiag) < 0.05, 0.05, offdiag)
    diagonal = 1.0 + jax.random.uniform(second_key, (LEV, LEV), jnp.float32, 0.0, 0.5)
    return jnp.where(distance == 0, diagonal, jnp.where(distance <= HB, offdiag, 0.0)).astype(jnp.float32)


def draw_stencil(key, part):
    row_key, col_key = jax.random.split(key)
    local = jnp.arange(NF, dtype=jnp.int32) % NFD
    fine_row = local // (4 * CW)
    fine_col = local % (4 * CW)
    row_base = jnp.clip((fine_row - 2) // 4 + jax.random.randint(row_key, (NF,), -1, 2), -1, CR - 1)
    col_base = jnp.clip((fine_col - 2) // 4 + jax.random.randint(col_key, (NF,), -1, 2), 0, CW - 2)
    corner = (row_base + 1) * CW + col_base
    return jnp.stack([corner, corner + 1, corner + CW, corner + CW + 1]).astype(jnp.int32)


def draw_interp_w(key, part):
    along_key, across_key = jax.random.split(key)
    along = jax.random.uniform(along_key, (NF,), jnp.float32)
    across = jax.random.uniform(across_key, (NF,), jnp.float32)
    weights = jnp.stack([(1.0 - along) * (1.0 - across), along * (1.0 - across), (1.0 - along) * across, along * across])
    return weights.astype(jnp.bfloat16)


def shard_levels(key, dims, pieces, low, top_value):
    gain = 1.0
    for dim, parts in pieces:
        heights = jax.random.uniform(jax.random.fold_in(jax.random.fold_in(key, 6), dim), (parts,), jnp.float32, low / len(pieces), top_value / len(pieces))
        gain = gain * jnp.repeat(jnp.exp(heights), dims[dim] // parts).reshape((-1,) + (1,) * (len(dims) - 1 - dim))
    return gain


def noise(own_key, shape, spread, reach, shards=(), kind=jnp.bfloat16):
    array = spread * jax.random.normal(own_key, shape, jnp.float32)
    if shards:
        array = array * shard_levels(own_key, shape, shards, -0.22, 0.18)
    return jnp.clip(array, -reach, reach).astype(kind)


def setup_inputs(seed: int = 0) -> dict:
    splits = jax.random.split(jax.random.key(seed), 8)
    members_pert = noise(splits[0], (LEV, MEMBERS, NF), 0.3, 4.0, ((0, 4), (2, 8)))
    coarse_pert = noise(splits[1], (LEV, COARSE_MEMBERS, NC), 0.4, 6.0, ((0, 4), (2, 8)))
    member_ctrl = noise(splits[2], (LEV, MEMBERS, NC), 1.0, 6.0, ((0, 4), (2, 8)))
    coarse_ctrl = noise(splits[3], (LEV, COARSE_MEMBERS, NC), 1.0, 6.0, ((0, 4), (2, 8)))
    vert_loc = draw_vert_loc(jax.random.fold_in(splits[7], 71), 0)
    stencil = draw_stencil(jax.random.fold_in(splits[7], 71), 0)
    interp_w = draw_interp_w(jax.random.fold_in(splits[7], 71), 0)
    return {"members_pert": members_pert, "coarse_pert": coarse_pert, "member_ctrl": member_ctrl, "coarse_ctrl": coarse_ctrl, "vert_loc": vert_loc, "stencil": stencil, "interp_w": interp_w}


def reference(members_pert, coarse_pert, member_ctrl, coarse_ctrl, vert_loc, stencil, interp_w):
    highest = lax.Precision.HIGHEST
    loc_members = jnp.einsum("ij,jkc->ikc", vert_loc, member_ctrl.astype(jnp.float32), precision=highest).astype(jnp.bfloat16)
    loc_coarse = jnp.einsum("ij,jkc->ikc", vert_loc, coarse_ctrl.astype(jnp.float32), precision=highest).astype(jnp.bfloat16)
    combined = jnp.sum(coarse_pert.astype(jnp.float32) * loc_coarse.astype(jnp.float32), axis=1).astype(jnp.bfloat16)
    fields = jnp.concatenate([loc_members, combined[:, None, :]], axis=1)
    levels = fields.shape[0]
    kinds = fields.shape[1]
    blocks = fields.reshape(levels, kinds, N_TILE, NCD)
    window = jnp.concatenate([jnp.roll(blocks, 1, axis=2)[..., NCD - CW:], blocks, jnp.roll(blocks, -1, axis=2)[..., :CW]], axis=3)
    window = jnp.moveaxis(window, 2, 0)
    window_span = window.shape[3]

    def one_tile(tile_index):
        local_window = lax.dynamic_index_in_dim(window, tile_index, 0, keepdims=False)
        first = (tile_index * NFD).astype(jnp.int32)
        corners = lax.dynamic_slice_in_dim(stencil, first, NFD, 1)
        weights = lax.dynamic_slice_in_dim(interp_w, first, NFD, 1).astype(jnp.float32)
        pert = lax.dynamic_slice_in_dim(members_pert, first, NFD, 2).astype(jnp.float32)
        interp = jnp.zeros((levels, kinds, NFD), jnp.float32)
        for corner in range(4):
            interp = interp + weights[corner][None, None, :] * local_window[:, :, corners[corner]].astype(jnp.float32)
        increment = jnp.sum(pert * interp[:, :MEMBERS], axis=1) + interp[:, MEMBERS]
        adjoint = jnp.concatenate([pert * increment[:, None, :], increment[:, None, :]], axis=1)
        adjoint = adjoint.astype(jnp.bfloat16).astype(jnp.float32)
        coarse_adjoint = jnp.zeros((levels, kinds, window_span), jnp.float32)
        for corner in range(4):
            coarse_adjoint = coarse_adjoint.at[:, :, corners[corner]].add(weights[corner][None, None, :] * adjoint)
        return coarse_adjoint

    backs = lax.map(one_tile, jnp.arange(N_TILE, dtype=jnp.int32))
    own_cells = backs[..., CW:CW + NCD]
    left_rim = backs[..., :CW]
    right_rim = backs[..., CW + NCD:]
    own_cells = own_cells.at[..., NCD - CW:].add(jnp.roll(left_rim, -1, axis=0))
    own_cells = own_cells.at[..., :CW].add(jnp.roll(right_rim, 1, axis=0))
    gathered = jnp.moveaxis(own_cells, 0, 2).reshape(levels, kinds, N_TILE * NCD)
    adjoint_ctrl = jnp.concatenate([gathered[:, :MEMBERS], coarse_pert.astype(jnp.float32) * gathered[:, MEMBERS:MEMBERS + 1]], axis=1)
    result = jnp.einsum("ij,ikc->jkc", vert_loc, adjoint_ctrl, precision=highest)
    return result[:, :MEMBERS], result[:, MEMBERS:]
```

```python
import functools

import jax
import jax.numpy as jnp
from jax import lax
from jax.experimental import pallas as pl
from jax.experimental.pallas import tpu as pltpu
from jax.sharding import PartitionSpec as P

HB = 4
CW = 64
LANE = 128
CHUNK = 1024
MESH = pl.DeviceIdType.MESH
F32 = jnp.float32
BF16 = jnp.bfloat16

DIRECTIONS = ((-1, -1), (1, -1), (-1, 1), (1, 1), (0, -1), (0, 1), (-1, 0), (1, 0))


def kernel(
    tiles, levs, pert_hbm, cp_hbm, mc_hbm, cc_hbm, vert_hbm, st_hbm, w_hbm, mo_ref, co_ref,
    mc, cc, cp, pert, vert, st, w, matrix, fld, comb, adj, inc, acc, out_buf, r_tile, r_lev, r_diag,
    mo, co, load_sem, send1, recv1, send2, recv2, store_sem,
):
    rows, members, cells = mc_hbm.shape
    group = cc_hbm.shape[1]
    total_levels = vert_hbm.shape[0]
    fine = pert_hbm.shape[2]
    span = cells + LANE
    edge = HB * members + rows
    comb_at = (rows - HB) * members
    tail_at = comb_at - HB * members

    def level_at(i):
        return (i - HB) * members if i >= HB else comb_at + rows + i * members

    t = lax.axis_index("tile")
    v = lax.axis_index("lev")
    first = v * rows
    has = {-1: v > 0, 0: None, 1: v < levs - 1}

    def when(dl, action):
        if dl == 0:
            action()
        else:
            pl.when(has[dl])(action)

    def device(dt, dl):
        return (lax.rem(t + dt + tiles, tiles), lax.rem(v + dl + levs, levs))

    own = pl.ds(HB, rows)
    loads = [
        pltpu.make_async_copy(mc_hbm, mc.at[own, :, pl.ds(0, cells)], load_sem.at[0]),
        pltpu.make_async_copy(cc_hbm, cc.at[own, :, pl.ds(0, cells)], load_sem.at[1]),
        pltpu.make_async_copy(cp_hbm, cp.at[own, :, pl.ds(0, cells)], load_sem.at[2]),
        pltpu.make_async_copy(st_hbm, st, load_sem.at[3]),
        pltpu.make_async_copy(w_hbm, w, load_sem.at[4]),
        pltpu.make_async_copy(vert_hbm, vert, load_sem.at[5]),
        pltpu.make_async_copy(pert_hbm, pert, load_sem.at[6]),
    ]
    for load in loads:
        load.start()

    barrier = pltpu.get_barrier_semaphore()
    for dt, dl in DIRECTIONS:
        when(
            dl,
            lambda dt=dt, dl=dl: pl.semaphore_signal(
                barrier, inc=1, device_id=device(dt, dl), device_id_type=MESH
            ),
        )

    level_src = {0: (HB, rows), 1: (rows, HB), -1: (HB, HB)}
    level_dst = {0: HB, 1: 0, -1: HB + rows}
    lane_src = {0: (0, cells), 1: (cells - LANE, LANE), -1: (0, LANE)}
    lane_dst = {0: 0, 1: cells + LANE, -1: cells}
    round1 = []
    for dt, dl in DIRECTIONS:
        for buf in (mc, cc, cp):
            if buf is cp and dt != 0 and dl != 0:
                continue
            n = len(round1)
            (l0, ln), (c0, cn) = level_src[dl], lane_src[dt]
            copy = pltpu.make_async_remote_copy(
                src_ref=buf.at[pl.ds(l0, ln), :, pl.ds(c0, cn)],
                dst_ref=buf.at[pl.ds(level_dst[dl], ln), :, pl.ds(lane_dst[dt], cn)],
                send_sem=send1.at[n],
                recv_sem=recv1.at[n],
                device_id=device(dt, dl),
                device_id_type=MESH,
            )
            round1.append((dl, copy))

    @pl.when(v == 0)
    def _():
        for buf in (mc, cc, cp):
            buf[0:HB] = jnp.zeros((HB,) + buf.shape[1:], BF16)
        r_lev[0] = jnp.zeros(r_lev.shape[1:], BF16)
        r_diag[0] = jnp.zeros(r_diag.shape[1:], BF16)

    @pl.when(v == levs - 1)
    def _():
        for buf in (mc, cc, cp):
            buf[HB + rows :] = jnp.zeros((HB,) + buf.shape[1:], BF16)
        r_lev[1] = jnp.zeros(r_lev.shape[1:], BF16)
        r_diag[1] = jnp.zeros(r_diag.shape[1:], BF16)

    for load in loads[:3]:
        load.wait()
    neighbours = 2 + 3 * jnp.where(v > 0, 1, 0) + 3 * jnp.where(v < levs - 1, 1, 0)
    pl.semaphore_wait(barrier, neighbours)
    for dl, copy in round1:
        when(dl, copy.start)

    for load in loads[3:6]:
        load.wait()
    pack = 16
    base_rows = lax.broadcasted_iota(jnp.int32, (pack, LANE), 0).astype(jnp.int16)

    def build(step, carry):
        lanes = pl.ds(pl.multiple_of(step * LANE, LANE), LANE)
        places, weights = [], []
        for corner in range(4):
            cell = st[corner : corner + 1, lanes] - CW
            cell = jnp.where(cell < 0, cell + span, cell)
            places.append(jnp.broadcast_to(cell, (pack, LANE)).astype(jnp.int16))
            weight = w[corner : corner + 1, lanes].astype(F32)
            weights.append(jnp.broadcast_to(weight, (pack, LANE)).astype(BF16))
        for block in range(span // pack):
            index = base_rows + jnp.int16(block * pack)
            value = jnp.zeros((pack, LANE), BF16)
            for corner in range(4):
                value = jnp.where(places[corner] == index, weights[corner], value)
            matrix[block * pack : (block + 1) * pack, lanes] = value
        return carry

    lax.fori_loop(0, fine // LANE, build, 0)

    for dl, copy in round1:
        when(-dl, copy.wait_recv)

    next_side = lax.broadcasted_iota(jnp.int32, (1, LANE), 1) < LANE - CW

    def window(buf, level, lane_tile):
        if lane_tile * LANE < cells:
            return buf[level, :, lane_tile * LANE : (lane_tile + 1) * LANE].astype(F32)
        from_next = buf[level, :, cells : cells + LANE].astype(F32)
        from_prev = buf[level, :, cells + LANE : cells + 2 * LANE].astype(F32)
        return jnp.where(next_side, from_next, from_prev)

    def factor(i, j):
        return vert[
            lax.rem(first + i + total_levels, total_levels),
            lax.rem(first + j + total_levels, total_levels),
        ]

    for lane_tile in range(span // LANE):
        lanes = slice(lane_tile * LANE, (lane_tile + 1) * LANE)
        values = [window(mc, level, lane_tile) for level in range(rows + 2 * HB)]
        for i in range(rows):
            total = factor(i, i - HB) * values[i]
            for d in range(1, 2 * HB + 1):
                total = total + factor(i, i + d - HB) * values[i + d]
            at = level_at(i)
            fld[at : at + members, lanes] = total.astype(BF16)
        values = [window(cc, level, lane_tile) for level in range(rows + 2 * HB)]
        for i in range(rows):
            total = factor(i, i - HB) * values[i]
            for d in range(1, 2 * HB + 1):
                total = total + factor(i, i + d - HB) * values[i + d]
            total = total.astype(BF16).astype(F32) * window(cp, i + HB, lane_tile)
            comb[i : i + 1, lanes] = jnp.sum(total, axis=0, keepdims=True)
    fld[comb_at : comb_at + rows, :] = comb[...].astype(BF16)

    loads[6].wait()
    for chunk in range(fine // CHUNK):
        lanes = slice(chunk * CHUNK, (chunk + 1) * CHUNK)
        interp = jnp.dot(fld[...], matrix[:, lanes], preferred_element_type=F32)
        for i in range(rows):
            at = level_at(i)
            member = pert[i, :, lanes].astype(F32)
            line = jnp.sum(member * interp[at : at + members], axis=0, keepdims=True)
            line = line + interp[comb_at + i : comb_at + i + 1]
            adj[at : at + members, lanes] = (member * line).astype(BF16)
            inc[i : i + 1, lanes] = line
        adj[comb_at : comb_at + rows, lanes] = inc[:, lanes].astype(BF16)
        back = lax.dot_general(
            adj[:, lanes], matrix[:, lanes], (((1,), (1,)), ((), ())), preferred_element_type=F32
        )
        if chunk == 0:
            acc[...] = back
        else:
            acc[...] += back
    out_buf[...] = acc[...].astype(BF16)

    row_src = {0: (0, acc.shape[0]), 1: (tail_at, edge), -1: (comb_at, edge)}
    round2 = []
    for n, (dt, dl) in enumerate(DIRECTIONS):
        r0, rn = row_src[dl]
        side, floor = (1 - dt) // 2, (1 - dl) // 2
        if dt == 0:
            src, dst = out_buf.at[pl.ds(r0, rn), pl.ds(0, cells)], r_lev.at[floor]
        else:
            src = out_buf.at[pl.ds(r0, rn), pl.ds(cells, LANE)]
            dst = r_tile.at[side] if dl == 0 else r_diag.at[floor, side]
        copy = pltpu.make_async_remote_copy(
            src_ref=src,
            dst_ref=dst,
            send_sem=send2.at[n],
            recv_sem=recv2.at[n],
            device_id=device(dt, dl),
            device_id_type=MESH,
        )
        round2.append((dl, copy))
    for dl, copy in round2:
        when(dl, copy.start)
    for dl, copy in round2:
        when(-dl, copy.wait_recv)

    tile_lanes = lax.broadcasted_iota(jnp.int32, (1, LANE), 1)
    for lane_tile in range(cells // LANE):
        lanes = slice(lane_tile * LANE, (lane_tile + 1) * LANE)

        def joined(base, prev, following):
            if lane_tile == 0:
                base = base + jnp.where(tile_lanes < CW, prev.astype(F32), 0.0)
            if lane_tile == cells // LANE - 1:
                base = base + jnp.where(tile_lanes >= LANE - CW, following.astype(F32), 0.0)
            return base

        def halo(floor, r0, rn):
            at = slice(r0, r0 + rn)
            return joined(
                r_lev[floor, at, lanes].astype(F32), r_diag[floor, 0, at, :], r_diag[floor, 1, at, :]
            )

        def inner(r0, rn):
            at = slice(r0, r0 + rn)
            return joined(acc[at, lanes], r_tile[0, at, :], r_tile[1, at, :])

        values = [halo(0, i * members, members) for i in range(HB)]
        values += [inner(level_at(i), members) for i in range(rows)]
        values += [halo(1, rows + i * members, members) for i in range(HB)]
        for j in range(rows):
            total = factor(j - HB, j) * values[j]
            for d in range(1, 2 * HB + 1):
                total = total + factor(j + d - HB, j) * values[j + d]
            mo[j, :, lanes] = total
        below = halo(0, HB * members, rows)
        middle = inner(comb_at, rows)
        above = halo(1, 0, rows)
        lines = [below[rows - HB + i : rows - HB + i + 1] for i in range(HB)]
        lines += [middle[i : i + 1] for i in range(rows)]
        lines += [above[i : i + 1] for i in range(HB)]
        values = [
            cp[level, :, lanes].astype(F32) * lines[level] for level in range(rows + 2 * HB)
        ]
        for j in range(rows):
            total = factor(j - HB, j) * values[j]
            for d in range(1, 2 * HB + 1):
                total = total + factor(j + d - HB, j) * values[j + d]
            co[j, :, lanes] = total

    stores = [
        pltpu.make_async_copy(mo, mo_ref, store_sem.at[0]),
        pltpu.make_async_copy(co, co_ref, store_sem.at[1]),
    ]
    for store in stores:
        store.start()
    for dl, copy in round1 + round2:
        when(dl, copy.wait_send)
    for store in stores:
        store.wait()


def solution(mesh):
    tiles, levs = mesh.shape["tile"], mesh.shape["lev"]

    def step(members_pert, coarse_pert, member_ctrl, coarse_ctrl, vert_loc, stencil, interp_w):
        rows, members, cells = member_ctrl.shape
        group = coarse_ctrl.shape[1]
        fine = members_pert.shape[2]
        levels, span, lines = rows + 2 * HB, cells + LANE, rows * (members + 1)
        edge = HB * members + rows
        hbm = pl.BlockSpec(memory_space=pl.ANY)
        copies = 8 * 2 + 4
        return pl.pallas_call(
            functools.partial(kernel, tiles, levs),
            out_shape=(
                jax.ShapeDtypeStruct((rows, members, cells), F32),
                jax.ShapeDtypeStruct((rows, group, cells), F32),
            ),
            in_specs=[hbm] * 7,
            out_specs=(hbm, hbm),
            scratch_shapes=[
                pltpu.VMEM((levels, members, cells + 2 * LANE), BF16),
                pltpu.VMEM((levels, group, cells + 2 * LANE), BF16),
                pltpu.VMEM((levels, group, cells + 2 * LANE), BF16),
                pltpu.VMEM((rows, members, fine), BF16),
                pltpu.SMEM(vert_loc.shape, F32),
                pltpu.VMEM(stencil.shape, jnp.int32),
                pltpu.VMEM(interp_w.shape, BF16),
                pltpu.VMEM((span, fine), BF16),
                pltpu.VMEM((lines, span), BF16),
                pltpu.VMEM((rows, span), F32),
                pltpu.VMEM((lines, fine), BF16),
                pltpu.VMEM((rows, fine), F32),
                pltpu.VMEM((lines, span), F32),
                pltpu.VMEM((lines, span), BF16),
                pltpu.VMEM((2, lines, LANE), BF16),
                pltpu.VMEM((2, edge, cells), BF16),
                pltpu.VMEM((2, 2, edge, LANE), BF16),
                pltpu.VMEM((rows, members, cells), F32),
                pltpu.VMEM((rows, group, cells), F32),
                pltpu.SemaphoreType.DMA((7,)),
                pltpu.SemaphoreType.DMA((copies,)),
                pltpu.SemaphoreType.DMA((copies,)),
                pltpu.SemaphoreType.DMA((8,)),
                pltpu.SemaphoreType.DMA((8,)),
                pltpu.SemaphoreType.DMA((2,)),
            ],
            compiler_params=pltpu.CompilerParams(
                collective_id=0, has_side_effects=True, vmem_limit_bytes=60 * 1024 * 1024
            ),
        )(members_pert, coarse_pert, member_ctrl, coarse_ctrl, vert_loc, stencil, interp_w)

    in_specs = (
        P("lev", None, "tile"),
        P("lev", None, "tile"),
        P("lev", None, "tile"),
        P("lev", None, "tile"),
        P(),
        P(None, "tile"),
        P(None, "tile"),
    )
    out_specs = (P("lev", None, "tile"), P("lev", None, "tile"))
    return jax.shard_map(step, mesh=mesh, in_specs=in_specs, out_specs=out_specs, check_vma=False)
```

```python
import functools

import jax
import jax.numpy as jnp
from jax import lax
from jax.experimental import pallas as pl
from jax.experimental.pallas import tpu as pltpu
from jax.sharding import PartitionSpec as P

HB = 4
CW = 64
LANE = 128
CHUNK = 1024
MESH = pl.DeviceIdType.MESH
F32 = jnp.float32
BF16 = jnp.bfloat16

DIRECTIONS = ((0, -1), (0, 1), (-1, 0), (1, 0), (-1, -1), (1, -1), (-1, 1), (1, 1))


def kernel(
    tiles, levs, pert_hbm, cp_hbm, mc_hbm, cc_hbm, vert_hbm, st_hbm, w_hbm, mo, co,
    mc, cc, cp, pert, vert, st, w, matrix, fld, comb, adj, inc, acc, out_buf, r_tile, r_lev, r_diag,
    load_sem, send1, recv1, send2, recv2,
):
    rows, members, cells = mc_hbm.shape
    group = cc_hbm.shape[1]
    total_levels = vert_hbm.shape[0]
    fine = pert_hbm.shape[2]
    span = cells + LANE
    edge = HB * members + rows
    comb_at = (rows - HB) * members
    tail_at = comb_at - HB * members

    def level_at(i):
        return (i - HB) * members if i >= HB else comb_at + rows + i * members

    t = lax.axis_index("tile")
    v = lax.axis_index("lev")
    first = v * rows
    has = {-1: v > 0, 0: None, 1: v < levs - 1}

    def when(dl, action):
        if dl == 0:
            action()
        else:
            pl.when(has[dl])(action)

    def device(dt, dl):
        return (lax.rem(t + dt + tiles, tiles), lax.rem(v + dl + levs, levs))

    own = pl.ds(HB, rows)
    loads = [
        pltpu.make_async_copy(mc_hbm, mc.at[own, :, pl.ds(0, cells)], load_sem.at[0]),
        pltpu.make_async_copy(cc_hbm, cc.at[own, :, pl.ds(0, cells)], load_sem.at[1]),
        pltpu.make_async_copy(cp_hbm, cp.at[own, :, pl.ds(0, cells)], load_sem.at[2]),
        pltpu.make_async_copy(st_hbm, st, load_sem.at[3]),
        pltpu.make_async_copy(w_hbm, w, load_sem.at[4]),
        pltpu.make_async_copy(vert_hbm, vert, load_sem.at[5]),
        pltpu.make_async_copy(pert_hbm, pert, load_sem.at[6]),
    ]
    for load in loads:
        load.start()

    barrier = pltpu.get_barrier_semaphore()
    for dt, dl in DIRECTIONS:
        when(
            dl,
            lambda dt=dt, dl=dl: pl.semaphore_signal(
                barrier, inc=1, device_id=device(dt, dl), device_id_type=MESH
            ),
        )

    level_src = {0: (HB, rows), 1: (rows, HB), -1: (HB, HB)}
    level_dst = {0: HB, 1: 0, -1: HB + rows}
    lane_src = {0: (0, cells), 1: (cells - LANE, LANE), -1: (0, LANE)}
    lane_dst = {0: 0, 1: cells + LANE, -1: cells}
    wanted = [(buf, direction) for direction in DIRECTIONS for buf in (mc, cc)]
    wanted += [(cp, direction) for direction in ((-1, 0), (1, 0), (0, -1), (0, 1))]
    round1 = []
    for n, (buf, (dt, dl)) in enumerate(wanted):
        (l0, ln), (c0, cn) = level_src[dl], lane_src[dt]
        copy = pltpu.make_async_remote_copy(
            src_ref=buf.at[pl.ds(l0, ln), :, pl.ds(c0, cn)],
            dst_ref=buf.at[pl.ds(level_dst[dl], ln), :, pl.ds(lane_dst[dt], cn)],
            send_sem=send1.at[n],
            recv_sem=recv1.at[n],
            device_id=device(dt, dl),
            device_id_type=MESH,
        )
        round1.append((dl, copy))
    needed = {"own": round1[:4], "rim": round1[4:-2], "spread": round1[-2:]}

    def arrive(stage):
        for dl, copy in needed[stage]:
            when(-dl, copy.wait_recv)

    @pl.when(v == 0)
    def _():
        for buf in (mc, cc, cp):
            buf[0:HB] = jnp.zeros((HB,) + buf.shape[1:], BF16)
        r_lev[0] = jnp.zeros(r_lev.shape[1:], BF16)
        r_diag[0] = jnp.zeros(r_diag.shape[1:], BF16)

    @pl.when(v == levs - 1)
    def _():
        for buf in (mc, cc, cp):
            buf[HB + rows :] = jnp.zeros((HB,) + buf.shape[1:], BF16)
        r_lev[1] = jnp.zeros(r_lev.shape[1:], BF16)
        r_diag[1] = jnp.zeros(r_diag.shape[1:], BF16)

    for load in loads[:3]:
        load.wait()
    neighbours = 2 + 3 * jnp.where(v > 0, 1, 0) + 3 * jnp.where(v < levs - 1, 1, 0)
    pl.semaphore_wait(barrier, neighbours)
    for dl, copy in round1:
        when(dl, copy.start)

    for load in loads[3:6]:
        load.wait()
    pack = 16
    base_rows = lax.broadcasted_iota(jnp.int32, (pack, LANE), 0).astype(jnp.int16)

    def build(step, carry):
        lanes = pl.ds(pl.multiple_of(step * LANE, LANE), LANE)
        places, weights = [], []
        for corner in range(4):
            cell = st[corner : corner + 1, lanes] - CW
            cell = jnp.where(cell < 0, cell + span, cell)
            places.append(jnp.broadcast_to(cell, (pack, LANE)).astype(jnp.int16))
            weight = w[corner : corner + 1, lanes].astype(F32)
            weights.append(jnp.broadcast_to(weight, (pack, LANE)).astype(BF16))
        for block in range(span // pack):
            index = base_rows + jnp.int16(block * pack)
            value = jnp.zeros((pack, LANE), BF16)
            for corner in range(4):
                value = jnp.where(places[corner] == index, weights[corner], value)
            matrix[block * pack : (block + 1) * pack, lanes] = value
        return carry

    lax.fori_loop(0, fine // LANE, build, 0)

    next_side = lax.broadcasted_iota(jnp.int32, (1, LANE), 1) < LANE - CW

    def window(buf, level, lane_tile):
        if lane_tile * LANE < cells:
            return buf[level, :, lane_tile * LANE : (lane_tile + 1) * LANE].astype(F32)
        from_next = buf[level, :, cells : cells + LANE].astype(F32)
        from_prev = buf[level, :, cells + LANE : cells + 2 * LANE].astype(F32)
        return jnp.where(next_side, from_next, from_prev)

    def factor(i, j):
        return vert[
            lax.rem(first + i + total_levels, total_levels),
            lax.rem(first + j + total_levels, total_levels),
        ]

    for lane_tile in range(span // LANE):
        if lane_tile == 0:
            arrive("own")
        if lane_tile * LANE == cells:
            arrive("rim")
        lanes = slice(lane_tile * LANE, (lane_tile + 1) * LANE)
        values = [window(mc, level, lane_tile) for level in range(rows + 2 * HB)]
        for i in range(rows):
            total = factor(i, i - HB) * values[i]
            for d in range(1, 2 * HB + 1):
                total = total + factor(i, i + d - HB) * values[i + d]
            at = level_at(i)
            fld[at : at + members, lanes] = total.astype(BF16)
        values = [window(cc, level, lane_tile) for level in range(rows + 2 * HB)]
        for i in range(rows):
            total = factor(i, i - HB) * values[i]
            for d in range(1, 2 * HB + 1):
                total = total + factor(i, i + d - HB) * values[i + d]
            total = total.astype(BF16).astype(F32) * window(cp, i + HB, lane_tile)
            comb[i : i + 1, lanes] = jnp.sum(total, axis=0, keepdims=True)
    fld[comb_at : comb_at + rows, :] = comb[...].astype(BF16)

    loads[6].wait()
    for chunk in range(fine // CHUNK):
        lanes = slice(chunk * CHUNK, (chunk + 1) * CHUNK)
        interp = jnp.dot(fld[...], matrix[:, lanes], preferred_element_type=F32)
        for i in range(rows):
            at = level_at(i)
            member = pert[i, :, lanes].astype(F32)
            line = jnp.sum(member * interp[at : at + members], axis=0, keepdims=True)
            line = line + interp[comb_at + i : comb_at + i + 1]
            adj[at : at + members, lanes] = (member * line).astype(BF16)
            inc[i : i + 1, lanes] = line
        adj[comb_at : comb_at + rows, lanes] = inc[:, lanes].astype(BF16)
        back = lax.dot_general(
            adj[:, lanes], matrix[:, lanes], (((1,), (1,)), ((), ())), preferred_element_type=F32
        )
        if chunk == 0:
            acc[...] = back
        else:
            acc[...] += back
    out_buf[...] = acc[...].astype(BF16)

    row_src = {0: (0, acc.shape[0]), 1: (tail_at, edge), -1: (comb_at, edge)}
    round2 = []
    for n, (dt, dl) in enumerate(DIRECTIONS):
        r0, rn = row_src[dl]
        side, floor = (1 - dt) // 2, (1 - dl) // 2
        if dt == 0:
            src, dst = out_buf.at[pl.ds(r0, rn), pl.ds(0, cells)], r_lev.at[floor]
        else:
            src = out_buf.at[pl.ds(r0, rn), pl.ds(cells, LANE)]
            dst = r_tile.at[side] if dl == 0 else r_diag.at[floor, side]
        copy = pltpu.make_async_remote_copy(
            src_ref=src,
            dst_ref=dst,
            send_sem=send2.at[n],
            recv_sem=recv2.at[n],
            device_id=device(dt, dl),
            device_id_type=MESH,
        )
        round2.append((dl, copy))
    for dl, copy in round2:
        when(dl, copy.start)
    arrive("spread")
    for dl, copy in round2:
        when(-dl, copy.wait_recv)

    tile_lanes = lax.broadcasted_iota(jnp.int32, (1, LANE), 1)
    for lane_tile in range(cells // LANE):
        lanes = slice(lane_tile * LANE, (lane_tile + 1) * LANE)

        def joined(base, prev, following):
            if lane_tile == 0:
                base = base + jnp.where(tile_lanes < CW, prev.astype(F32), 0.0)
            if lane_tile == cells // LANE - 1:
                base = base + jnp.where(tile_lanes >= LANE - CW, following.astype(F32), 0.0)
            return base

        def halo(floor, r0, rn):
            at = slice(r0, r0 + rn)
            return joined(
                r_lev[floor, at, lanes].astype(F32), r_diag[floor, 0, at, :], r_diag[floor, 1, at, :]
            )

        def inner(r0, rn):
            at = slice(r0, r0 + rn)
            return joined(acc[at, lanes], r_tile[0, at, :], r_tile[1, at, :])

        values = [halo(0, i * members, members) for i in range(HB)]
        values += [inner(level_at(i), members) for i in range(rows)]
        values += [halo(1, rows + i * members, members) for i in range(HB)]
        for j in range(rows):
            total = factor(j - HB, j) * values[j]
            for d in range(1, 2 * HB + 1):
                total = total + factor(j + d - HB, j) * values[j + d]
            mo[j, :, lanes] = total
        below = halo(0, HB * members, rows)
        middle = inner(comb_at, rows)
        above = halo(1, 0, rows)
        lines = [below[rows - HB + i : rows - HB + i + 1] for i in range(HB)]
        lines += [middle[i : i + 1] for i in range(rows)]
        lines += [above[i : i + 1] for i in range(HB)]
        values = [
            cp[level, :, lanes].astype(F32) * lines[level] for level in range(rows + 2 * HB)
        ]
        for j in range(rows):
            total = factor(j - HB, j) * values[j]
            for d in range(1, 2 * HB + 1):
                total = total + factor(j + d - HB, j) * values[j + d]
            co[j, :, lanes] = total

    for dl, copy in round1 + round2:
        when(dl, copy.wait_send)


def store(mo, co, mo_hbm, co_hbm, sem):
    copies = [
        pltpu.make_async_copy(mo, mo_hbm, sem.at[0]),
        pltpu.make_async_copy(co, co_hbm, sem.at[1]),
    ]
    for copy in copies:
        copy.start()
    for copy in copies:
        copy.wait()


def solution(mesh):
    tiles, levs = mesh.shape["tile"], mesh.shape["lev"]

    def step(members_pert, coarse_pert, member_ctrl, coarse_ctrl, vert_loc, stencil, interp_w):
        rows, members, cells = member_ctrl.shape
        group = coarse_ctrl.shape[1]
        fine = members_pert.shape[2]
        levels, span, lines = rows + 2 * HB, cells + LANE, rows * (members + 1)
        edge = HB * members + rows
        hbm = pl.BlockSpec(memory_space=pl.ANY)
        copies = 8 * 2 + 4
        vmem = pl.BlockSpec(memory_space=pltpu.VMEM)
        results = pl.pallas_call(
            functools.partial(kernel, tiles, levs),
            out_shape=(
                pltpu.VMEM((rows, members, cells), F32),
                pltpu.VMEM((rows, group, cells), F32),
            ),
            in_specs=[hbm] * 7,
            out_specs=(vmem, vmem),
            scratch_shapes=[
                pltpu.VMEM((levels, members, cells + 2 * LANE), BF16),
                pltpu.VMEM((levels, group, cells + 2 * LANE), BF16),
                pltpu.VMEM((levels, group, cells + 2 * LANE), BF16),
                pltpu.VMEM((rows, members, fine), BF16),
                pltpu.SMEM(vert_loc.shape, F32),
                pltpu.VMEM(stencil.shape, jnp.int32),
                pltpu.VMEM(interp_w.shape, BF16),
                pltpu.VMEM((span, fine), BF16),
                pltpu.VMEM((lines, span), BF16),
                pltpu.VMEM((rows, span), F32),
                pltpu.VMEM((lines, fine), BF16),
                pltpu.VMEM((rows, fine), F32),
                pltpu.VMEM((lines, span), F32),
                pltpu.VMEM((lines, span), BF16),
                pltpu.VMEM((2, lines, LANE), BF16),
                pltpu.VMEM((2, edge, cells), BF16),
                pltpu.VMEM((2, 2, edge, LANE), BF16),
                pltpu.SemaphoreType.DMA((7,)),
                pltpu.SemaphoreType.DMA((copies,)),
                pltpu.SemaphoreType.DMA((copies,)),
                pltpu.SemaphoreType.DMA((8,)),
                pltpu.SemaphoreType.DMA((8,)),
            ],
            compiler_params=pltpu.CompilerParams(
                collective_id=0, has_side_effects=True, vmem_limit_bytes=60 * 1024 * 1024
            ),
        )(members_pert, coarse_pert, member_ctrl, coarse_ctrl, vert_loc, stencil, interp_w)
        return pl.pallas_call(
            store,
            out_shape=(
                jax.ShapeDtypeStruct((rows, members, cells), F32),
                jax.ShapeDtypeStruct((rows, group, cells), F32),
            ),
            in_specs=[vmem, vmem],
            out_specs=(hbm, hbm),
            scratch_shapes=[pltpu.SemaphoreType.DMA((2,))],
            compiler_params=pltpu.CompilerParams(vmem_limit_bytes=1024 * 1024),
        )(*results)

    in_specs = (
        P("lev", None, "tile"),
        P("lev", None, "tile"),
        P("lev", None, "tile"),
        P("lev", None, "tile"),
        P(),
        P(None, "tile"),
        P(None, "tile"),
    )
    out_specs = (P("lev", None, "tile"), P("lev", None, "tile"))
    return jax.shard_map(step, mesh=mesh, in_specs=in_specs, out_specs=out_specs, check_vma=False)
```
